32 devices in a mesh: dp: 1 (over z), tp: 32 (over x, y, core).
Axes of the slice: x: 4, y: 4, z: 1, core: 2. Of those that a mesh axis runs over, the one named last changes fastest.
The devices are a block of a 4x4x8 slice.
Arguments:
- x: bfloat16 [8192, 4096], P(('dp', 'tp'))
- dy: bfloat16 [8192, 4096], P(('dp', 'tp'))
- gate: bfloat16 [8192, 16384], P('dp', 'tp')
- up: bfloat16 [8192, 16384], P('dp', 'tp')
- w_gate: bfloat16 [4096, 16384], P(None, 'tp')
- w_up: bfloat16 [4096, 16384], P(None, 'tp')
- w_down: bfloat16 [16384, 4096], P('tp')
Outputs:
- output 1: bfloat16 [8192, 4096], P(('dp', 'tp'))
- output 2: bfloat16 [4096, 16384], P('dp', 'tp')
- output 3: bfloat16 [4096, 16384], P('dp', 'tp')
- output 4: bfloat16 [16384, 4096], P(('dp', 'tp'))
All inputs are finite; a program needn't handle non-finite values.
Results may differ from the reference program's by a relative error of at most 0.012.
Values are sent between devices in bfloat16 or wider.
A program may use at most 768 MiB of HBM per device.

```python
import jax
import jax.numpy as jnp

ROWS = 8192
D = 4096
FF = 16384


def act(gate, up):
    return jax.nn.silu(gate) * up


def setup_inputs(seed: int = 0, part: int = 0) -> dict:
    kx, ky, ka, kb, kg, ku, kd = jax.random.split(jax.random.key(seed), 7)
    kx, ky, ka, kb = (jax.random.fold_in(k, part) for k in (kx, ky, ka, kb))
    drawn = {
        "x": jax.random.normal(kx, (ROWS, D), jnp.float32),
        "dy": jax.random.normal(ky, (ROWS, D), jnp.float32),
        "gate": jax.random.normal(ka, (ROWS, FF), jnp.float32),
        "up": jax.random.normal(kb, (ROWS, FF), jnp.float32),
        "w_gate": jax.random.normal(kg, (D, FF), jnp.float32) * D**-0.5,
        "w_up": jax.random.normal(ku, (D, FF), jnp.float32) * D**-0.5,
        "w_down": jax.random.normal(kd, (FF, D), jnp.float32) * FF**-0.5,
    }
    return {k: v.astype(jnp.bfloat16) for k, v in drawn.items()}


def reference(x, dy, gate, up, w_gate, w_up, w_down):
    hidden, back = jax.vjp(act, gate.astype(jnp.float32), up.astype(jnp.float32))
    d_hidden = jnp.dot(dy, w_down.T, preferred_element_type=jnp.float32)
    d_gate, d_up = (g.astype(jnp.bfloat16) for g in back(d_hidden))
    dx = jnp.dot(d_gate, w_gate.T, preferred_element_type=jnp.float32) + jnp.dot(d_up, w_up.T, preferred_element_type=jnp.float32)
    dw_gate = jnp.dot(x.T, d_gate, preferred_element_type=jnp.float32)
    dw_up = jnp.dot(x.T, d_up, preferred_element_type=jnp.float32)
    dw_down = jnp.dot(hidden.astype(jnp.bfloat16).T, dy, preferred_element_type=jnp.float32)
    return tuple(g.astype(jnp.bfloat16) for g in (dx, dw_gate, dw_up, dw_down))
```

```python
import functools
import math

import jax
import jax.numpy as jnp
from jax import lax
from jax.experimental import pallas as pl
from jax.experimental.pallas import tpu as pltpu
from jax.sharding import PartitionSpec as P

MESH = pl.DeviceIdType.MESH
F32 = jnp.float32
BF16 = jnp.bfloat16
T_RHS = (((1,), (1,)), ((), ()))


def dot(a, b):
    return jnp.dot(a, b, preferred_element_type=F32)


def dot_t(a, b):
    return lax.dot_general(a, b, T_RHS, preferred_element_type=F32)


def kernel(
    side, tile,
    x_in, dy_in, gate, up, w_gate, w_up, w_down,
    dx_out, dwg_out, dwu_out, dwd_out, xg, dyg, sums, partner_sums,
    wg, wu, wd, acc_g, acc_u, acc_d, dyb, xb, gb, ub, dg, du, hid_t, dg_t, du_t, dg0, du0, to_partner, to_ring,
    load, loadw, loadx,
    dy_s, dy_r, dy_ps, dy_pr, x_s, x_r, x_ps, x_pr, rs_s, rs_r, ps_s, ps_r,
):
    n = side * side
    rows, depth = x_in.shape
    half = rows // 2
    ff = gate.shape[1]
    tiles = depth // tile

    me = lax.axis_index("tp")
    core = lax.rem(me, 2)
    chip = lax.div(me, 2)
    cx, cy = lax.div(chip, side), lax.rem(chip, side)
    diagonal = lax.rem(cx + cy, side)

    def device(c, q):
        major = lax.div(q, side)
        minor = lax.rem(lax.rem(q, side) - major + side, side)
        x = major + c * (minor - major)
        y = minor + c * (major - minor)
        return (x * side + y) * 2 + c

    other = 1 - core
    place = (cx + core * (cy - cx)) * side + diagonal
    other_place = (cx + other * (cy - cx)) * side + diagonal
    right = device(core, lax.rem(place + 1, n))
    left = device(core, lax.rem(place + n - 1, n))
    partner = me + 1 - 2 * core
    onward = (right, left)

    def piece(s, i):
        c, at = (core, place) if i < 2 else (other, other_place)
        q = lax.rem(at + n - s, n) if i % 2 == 0 else lax.rem(at + s, n)
        return pl.multiple_of(device(c, q) * rows + (i % 2) * half, half)

    def remote(src, dst, send, recv, to):
        return pltpu.make_async_remote_copy(
            src_ref=src, dst_ref=dst, send_sem=send, recv_sem=recv, device_id={"tp": to}, device_id_type=MESH
        )

    def columns(j):
        return pl.ds(pl.multiple_of(j * tile, tile), tile)

    def forward(src, whole, s, d, sems):
        at = whole.at[pl.ds(piece(s, d), half)]
        return remote(src, at, sems[0].at[d, s], sems[1].at[d, s + 1], onward[d])

    def across(src, whole, s, d, sems):
        at = whole.at[pl.ds(piece(s, d), half)]
        return remote(src, at, sems[2].at[d, s], sems[3].at[d, s], partner)

    def arrived(whole, s, d, sems):
        at = whole.at[pl.ds(piece(s, d), half)]
        return remote(at, at, sems[0].at[d, s], sems[1].at[d, s], onward[d])

    def arrived_across(whole, s, d, sems):
        at = whole.at[pl.ds(piece(s, 2 + d), half)]
        return remote(at, at, sems[2].at[d, s], sems[3].at[d, s], partner)

    def chunk_load(src, buf, i, sem):
        return pltpu.make_async_copy(src, buf.at[pl.ds(i * half, half)], sem.at[i])

    def gather_step(mine, whole, buf, s, sems, sem):
        for d in range(2):

            @pl.when(s == 0)
            def _():
                src = mine.at[pl.ds(d * half, half)]
                forward(src, whole, s, d, sems).start()
                across(src, whole, s, d, sems).start()
                chunk_load(src, buf, d, sem).start()

            @pl.when(s > 0)
            def _():
                arrived(whole, s, d, sems).wait_recv()
                src = whole.at[pl.ds(piece(s, d), half)]

                @pl.when(s < n - 1)
                def _():
                    forward(src, whole, s, d, sems).start()

                across(src, whole, s, d, sems).start()
                chunk_load(src, buf, d, sem).start()

    def gather_rest(whole, buf, s, sems, sem):
        for d in range(2):
            arrived_across(whole, s, d, sems).wait_recv()
            chunk_load(whole.at[pl.ds(piece(s, 2 + d), half)], buf, 2 + d, sem).start()
        for i in range(4):
            chunk_load(whole.at[pl.ds(piece(s, i), half)], buf, i, sem).wait()

    dy_sems = (dy_s, dy_r, dy_ps, dy_pr)
    x_sems = (x_s, x_r, x_ps, x_pr)

    def across_sum(s):
        return remote(to_partner, partner_sums.at[s], ps_s.at[s], ps_r.at[s], partner)

    def ring_sum(s, d):
        src = to_ring.at[pl.ds(d * half, half)]
        return remote(src, sums.at[s, d], rs_s.at[d, s], rs_r.at[d, s], onward[d])

    def term(a_gate, a_up, cols):
        return dot_t(a_gate, wg[cols, :]) + dot_t(a_up, wu[cols, :])

    def weight_loads():
        return [pltpu.make_async_copy(src, dst, loadw.at[i]) for i, (src, dst) in enumerate(((w_down, wd), (w_gate, wg), (w_up, wu)))]

    barrier = pltpu.get_barrier_semaphore()
    for peer in (left, right, partner):
        pl.semaphore_signal(barrier, inc=1, device_id={"tp": peer}, device_id_type=MESH)
    pl.semaphore_wait(barrier, 3)

    def step(s, carry):
        kept = []
        for i in range(4):
            at = pl.ds(piece(s, i), half)
            kept.append(pltpu.make_async_copy(gate.at[at], gb.at[pl.ds(i * half, half)], load.at[4 + i]))
            kept.append(pltpu.make_async_copy(up.at[at], ub.at[pl.ds(i * half, half)], load.at[8 + i]))
        gather_step(dy_in, dyg, dyb, s, dy_sems, load)
        for copy in kept:
            copy.start()

        @pl.when(s == 0)
        def _():
            for copy in weight_loads():
                copy.start()

            def clear(j, carry):
                zero = jnp.zeros((ff, tile), F32)
                for acc in (acc_g, acc_u, acc_d):
                    acc[:, columns(j)] = zero
                return carry

            gather_step(x_in, xg, xb, s, x_sems, loadx)
            lax.fori_loop(0, tiles, clear, 0)
            for copy in weight_loads():
                copy.wait()

        gather_rest(dyg, dyb, s, dy_sems, load)
        for copy in kept:
            copy.wait()

        ff_tile = min(256, ff)

        def activate(j, carry):
            cols = pl.ds(pl.multiple_of(j * ff_tile, ff_tile), ff_tile)
            d_hidden = dot_t(dyb[...], wd[cols, :])
            g, u = gb[:, cols].astype(F32), ub[:, cols].astype(F32)
            sig = jax.nn.sigmoid(g)
            silu = g * sig
            hid_t[cols, :] = (silu * u).astype(BF16).T
            d_up = (d_hidden * silu).astype(BF16)
            d_gate = ((d_hidden * u) * (sig * (1.0 + g * (1.0 - sig)))).astype(BF16)
            du[:, cols] = d_up
            dg[:, cols] = d_gate
            du_t[cols, :] = d_up.T
            dg_t[cols, :] = d_gate.T
            return carry

        lax.fori_loop(0, ff // ff_tile, activate, 0)

        @pl.when(s > 0)
        def _():
            across_sum(s - 1).wait_send()

        def for_partner(j, carry):
            cols = columns(j)
            to_partner[:, cols] = term(dg[rows:, :], du[rows:, :], cols).astype(BF16)
            return carry

        lax.fori_loop(0, tiles, for_partner, 0)
        across_sum(s).start()

        @pl.when(s > 0)
        def _():
            gather_step(x_in, xg, xb, s, x_sems, loadx)

        def down(j, carry):
            cols = columns(j)
            acc_d[:, cols] += dot(hid_t[...], dyb[:, cols])
            return carry

        lax.fori_loop(0, tiles, down, 0)

        @pl.when(s == 0)
        def _():
            dg0[...] = dg[:rows, :]
            du0[...] = du[:rows, :]

        @pl.when(s > 0)
        def _():
            across_sum(s).wait_recv()
            theirs = pltpu.make_async_copy(partner_sums.at[s], dyb.at[pl.ds(rows, rows)], load.at[2])
            theirs.start()

            @pl.when(s == 1)
            def _():
                dyb[:rows, :] = jnp.zeros((rows, depth), BF16)

            @pl.when(s > 1)
            def _():
                for d in range(2):
                    ring_sum(s - 1, d).wait_recv()
                    pltpu.make_async_copy(sums.at[s - 1, d], dyb.at[pl.ds(d * half, half)], load.at[d]).start()
                for d in range(2):
                    ring_sum(s - 1, d).wait_send()
                    pltpu.make_async_copy(sums.at[s - 1, d], dyb.at[pl.ds(d * half, half)], load.at[d]).wait()

            theirs.wait()

            def add(j, carry):
                cols = columns(j)
                total = term(dg[:rows, :], du[:rows, :], cols) + dyb[rows:, cols].astype(F32) + dyb[:rows, cols].astype(F32)
                to_ring[:, cols] = total.astype(BF16)
                return carry

            lax.fori_loop(0, tiles, add, 0)
            for d in range(2):
                ring_sum(s, d).start()

        gather_rest(xg, xb, s, x_sems, loadx)

        def gate_up(j, carry):
            cols = columns(j)
            acc_g[:, cols] += dot(dg_t[...], xb[:, cols])
            acc_u[:, cols] += dot(du_t[...], xb[:, cols])
            return carry

        lax.fori_loop(0, tiles, gate_up, 0)
        return carry

    lax.fori_loop(0, n, step, 0)

    across_sum(0).wait_recv()
    theirs = pltpu.make_async_copy(partner_sums.at[0], xb.at[pl.ds(0, rows)], load.at[2])
    theirs.start()

    def finish_down(j, carry):
        cols = columns(j)
        dyb[:, cols] = acc_d[:, cols].astype(BF16)
        return carry

    lax.fori_loop(0, tiles, finish_down, 0)
    out_d = pltpu.make_async_copy(dyb, dwd_out, load.at[3])
    out_d.start()
    theirs.wait()

    def own(j, carry):
        cols = columns(j)
        acc_d[:rows, cols] = term(dg0[...], du0[...], cols) + xb[:rows, cols].astype(F32)
        return carry

    lax.fori_loop(0, tiles, own, 0)

    def finish(acc, buf):
        def body(j, carry):
            cols = columns(j)
            buf[cols, :] = acc[:, cols].astype(BF16).T
            return carry

        lax.fori_loop(0, tiles, body, 0)

    finish(acc_g, wg)
    out_g = pltpu.make_async_copy(wg, dwg_out, load.at[4])
    out_g.start()
    finish(acc_u, wu)
    out_u = pltpu.make_async_copy(wu, dwu_out, load.at[5])
    out_u.start()

    last = []
    for d in range(2):
        ring_sum(n - 1, d).wait_recv()
        last.append(pltpu.make_async_copy(sums.at[n - 1, d], xb.at[pl.ds(rows + d * half, half)], load.at[d]))
        last[d].start()
    for d in range(2):
        ring_sum(n - 1, d).wait_send()
        last[d].wait()

    def finish_dx(j, carry):
        cols = columns(j)
        to_ring[:, cols] = (acc_d[:rows, cols] + xb[rows:, cols].astype(F32)).astype(BF16)
        return carry

    lax.fori_loop(0, tiles, finish_dx, 0)
    out_x = pltpu.make_async_copy(to_ring, dx_out, load.at[2])
    out_x.start()

    across_sum(n - 1).wait_send()

    def drain(s, carry):
        for mine, whole, sems in ((dy_in, dyg, dy_sems), (x_in, xg, x_sems)):
            for d in range(2):
                src = mine.at[pl.ds(d * half, half)]
                across(src, whole, s, d, sems).wait_send()

                @pl.when(s < n - 1)
                def _():
                    forward(src, whole, s, d, sems).wait_send()

        return carry

    lax.fori_loop(0, n, drain, 0)
    for copy in (out_d, out_g, out_u, out_x):
        copy.wait()


def solution(mesh):
    side = math.isqrt(mesh.shape["tp"] // 2)
    n = side * side
    assert 2 * n == mesh.shape["tp"]

    def step(x, dy, gate, up, w_gate, w_up, w_down):
        rows, depth = x.shape
        tokens, ff = gate.shape
        tile = min(512, depth)
        shape = jax.ShapeDtypeStruct
        any_space = pl.BlockSpec(memory_space=pl.ANY)
        dma = pltpu.SemaphoreType.DMA
        vmem = pltpu.VMEM
        outs = pl.pallas_call(
            functools.partial(kernel, side, tile),
            out_shape=[
                shape((rows, depth), BF16),
                shape((depth, ff), BF16),
                shape((depth, ff), BF16),
                shape((ff, depth), BF16),
                shape((tokens, depth), BF16),
                shape((tokens, depth), BF16),
                shape((n, 2, rows // 2, depth), BF16),
                shape((n, rows, depth), BF16),
            ],
            in_specs=[any_space] * 7,
            out_specs=[any_space] * 8,
            scratch_shapes=[
                vmem((depth, ff), BF16),
                vmem((depth, ff), BF16),
                vmem((ff, depth), BF16),
                vmem((ff, depth), F32),
                vmem((ff, depth), F32),
                vmem((ff, depth), F32),
                vmem((2 * rows, depth), BF16),
                vmem((2 * rows, depth), BF16),
                vmem((2 * rows, ff), BF16),
                vmem((2 * rows, ff), BF16),
                vmem((2 * rows, ff), BF16),
                vmem((2 * rows, ff), BF16),
                vmem((ff, 2 * rows), BF16),
                vmem((ff, 2 * rows), BF16),
                vmem((ff, 2 * rows), BF16),
                vmem((rows, ff), BF16),
                vmem((rows, ff), BF16),
                vmem((rows, depth), BF16),
                vmem((rows, depth), BF16),
                dma((12,)),
                dma((3,)),
                dma((4,)),
            ]
            + [dma((2, n)), dma((2, n + 1)), dma((2, n)), dma((2, n))] * 2
            + [dma((2, n)), dma((2, n)), dma((n,)), dma((n,))],
            compiler_params=pltpu.CompilerParams(
                collective_id=0, has_side_effects=True, vmem_limit_bytes=67_043_328
            ),
        )(x, dy, gate, up, w_gate, w_up, w_down)
        return tuple(outs[:4])

    tokens_spec = P(("dp", "tp"), None)
    return jax.shard_map(
        step,
        mesh=mesh,
        in_specs=(tokens_spec, tokens_spec, P("dp", "tp"), P("dp", "tp"), P(None, "tp"), P(None, "tp"), P("tp", None)),
        out_specs=(tokens_spec, P("dp", "tp"), P("dp", "tp"), tokens_spec),
        check_vma=False,
    )
```

```python
import functools
import math

import jax
import jax.numpy as jnp
from jax import lax
from jax.experimental import pallas as pl
from jax.experimental.pallas import tpu as pltpu
from jax.sharding import PartitionSpec as P

MESH = pl.DeviceIdType.MESH
F32 = jnp.float32
BF16 = jnp.bfloat16
T_RHS = (((1,), (1,)), ((), ()))


def dot(a, b):
    return jnp.dot(a, b, preferred_element_type=F32)


def dot_t(a, b):
    return lax.dot_general(a, b, T_RHS, preferred_element_type=F32)


def kernel(
    side, tile,
    x_in, dy_in, gate, up, w_gate, w_up, w_down,
    to_ring, wg, wu, dyb, xg, dyg, sums, partner_sums,
    wd, acc_g, acc_u, acc_d, xb, gb, ub, dg, du, hid_t, dg_t, du_t, to_partner, terms,
    load, loadw, loadx,
    dy_s, dy_r, dy_ps, dy_pr, x_s, x_r, x_ps, x_pr, rs_s, rs_r, ps_s, ps_r,
):
    n = side * side
    rows, depth = x_in.shape
    half = rows // 2
    quarter = half // 2
    ff = gate.shape[1]
    tiles = depth // tile

    me = lax.axis_index("tp")
    core = lax.rem(me, 2)
    chip = lax.div(me, 2)
    cx, cy = lax.div(chip, side), lax.rem(chip, side)
    diagonal = lax.rem(cx + cy, side)

    def device(c, q):
        major = lax.div(q, side)
        minor = lax.rem(lax.rem(q, side) - major + side, side)
        x = major + c * (minor - major)
        y = minor + c * (major - minor)
        return (x * side + y) * 2 + c

    other = 1 - core
    place = (cx + core * (cy - cx)) * side + diagonal
    other_place = (cx + other * (cy - cx)) * side + diagonal
    right = device(core, lax.rem(place + 1, n))
    left = device(core, lax.rem(place + n - 1, n))
    partner = me + 1 - 2 * core
    onward = (right, left)

    def piece(s, i):
        c, at = (core, place) if i < 2 else (other, other_place)
        q = lax.rem(at + n - s, n) if i % 2 == 0 else lax.rem(at + s, n)
        return pl.multiple_of(device(c, q) * rows + (i % 2) * half, half)

    def remote(src, dst, send, recv, to):
        return pltpu.make_async_remote_copy(
            src_ref=src, dst_ref=dst, send_sem=send, recv_sem=recv, device_id={"tp": to}, device_id_type=MESH
        )

    def columns(j):
        return pl.ds(pl.multiple_of(j * tile, tile), tile)

    def forward(src, whole, s, d, sems):
        at = whole.at[pl.ds(piece(s, d), half)]
        return remote(src, at, sems[0].at[d, s], sems[1].at[d, s + 1], onward[d])

    def across(src, whole, s, d, sems):
        at = whole.at[pl.ds(piece(s, d), half)]
        return remote(src, at, sems[2].at[d, s], sems[3].at[d, s], partner)

    def arrived(whole, s, d, sems):
        at = whole.at[pl.ds(piece(s, d), half)]
        return remote(at, at, sems[0].at[d, s], sems[1].at[d, s], onward[d])

    def arrived_across(whole, s, d, sems):
        at = whole.at[pl.ds(piece(s, 2 + d), half)]
        return remote(at, at, sems[2].at[d, s], sems[3].at[d, s], partner)

    def chunk_load(src, buf, i, sem):
        return pltpu.make_async_copy(src, buf.at[pl.ds(i * half, half)], sem.at[i])

    def gather_step(mine, whole, buf, s, sems, sem):
        for d in range(2):

            @pl.when(s == 0)
            def _():
                src = mine.at[pl.ds(d * half, half)]
                forward(src, whole, s, d, sems).start()
                across(src, whole, s, d, sems).start()
                chunk_load(src, buf, d, sem).start()

            @pl.when(s > 0)
            def _():
                arrived(whole, s, d, sems).wait_recv()
                src = whole.at[pl.ds(piece(s, d), half)]

                @pl.when(s < n - 1)
                def _():
                    forward(src, whole, s, d, sems).start()

                across(src, whole, s, d, sems).start()
                chunk_load(src, buf, d, sem).start()

    def gather_rest(whole, buf, s, sems, sem):
        for d in range(2):
            arrived_across(whole, s, d, sems).wait_recv()
            chunk_load(whole.at[pl.ds(piece(s, 2 + d), half)], buf, 2 + d, sem).start()
        for i in range(4):
            chunk_load(whole.at[pl.ds(piece(s, i), half)], buf, i, sem).wait()

    dy_sems = (dy_s, dy_r, dy_ps, dy_pr)
    x_sems = (x_s, x_r, x_ps, x_pr)

    def across_sum(s):
        return remote(to_partner, partner_sums.at[s], ps_s.at[s], ps_r.at[s], partner)

    def ring_sum(s, d, h):
        src = to_ring.at[pl.ds(d * half + h * quarter, quarter)]
        return remote(src, sums.at[s, d, h], rs_s.at[2 * d + h, s], rs_r.at[2 * d + h, s], onward[d])

    def add_arrived(s, term_slot, buf, send):
        def incoming(d, h):
            at = pl.ds(d * half + h * quarter, quarter)
            return pltpu.make_async_copy(sums.at[s, d, h], buf.at[at], load.at[d])

        for h in range(2):
            for d in range(2):
                ring_sum(s, d, h).wait_recv()
                incoming(d, h).start()
            for d in range(2):
                ring_sum(s, d, h).wait_send()
                incoming(d, h).wait()
                at = pl.ds(d * half + h * quarter, quarter)

                def add(j, carry):
                    cols = columns(j)
                    to_ring[at, cols] = (terms[term_slot, at, cols] + buf[at, cols].astype(F32)).astype(BF16)
                    return carry

                lax.fori_loop(0, tiles, add, 0)
                if send:
                    ring_sum(s + 1, d, h).start()

    def term(a_gate, a_up, cols):
        return dot_t(a_gate, wg[cols, :]) + dot_t(a_up, wu[cols, :])

    def weight_loads():
        return [pltpu.make_async_copy(src, dst, loadw.at[i]) for i, (src, dst) in enumerate(((w_down, wd), (w_gate, wg), (w_up, wu)))]

    barrier = pltpu.get_barrier_semaphore()
    for peer in (left, right, partner):
        pl.semaphore_signal(barrier, inc=1, device_id={"tp": peer}, device_id_type=MESH)
    pl.semaphore_wait(barrier, 3)

    def step(s, carry):
        kept = []
        for i in range(4):
            at = pl.ds(piece(s, i), half)
            kept.append(pltpu.make_async_copy(gate.at[at], gb.at[pl.ds(i * half, half)], load.at[4 + i]))
            kept.append(pltpu.make_async_copy(up.at[at], ub.at[pl.ds(i * half, half)], load.at[8 + i]))
        for copy in kept:
            copy.start()

        @pl.when(s != 1)
        def _():
            gather_step(dy_in, dyg, dyb, s, dy_sems, load)

        @pl.when(s == 0)
        def _():
            for copy in weight_loads():
                copy.start()

            def clear(j, carry):
                zero = jnp.zeros((ff, tile), F32)
                for acc in (acc_g, acc_u, acc_d):
                    acc[:, columns(j)] = zero
                return carry

            gather_step(x_in, xg, xb, s, x_sems, loadx)
            lax.fori_loop(0, tiles, clear, 0)
            for copy in weight_loads():
                copy.wait()

        gather_rest(dyg, dyb, s, dy_sems, load)
        for copy in kept:
            copy.wait()

        ff_tile = min(256, ff)

        def activate(j, carry):
            cols = pl.ds(pl.multiple_of(j * ff_tile, ff_tile), ff_tile)
            d_hidden = dot_t(dyb[...], wd[cols, :])
            g, u = gb[:, cols].astype(F32), ub[:, cols].astype(F32)
            sig = jax.nn.sigmoid(g)
            silu = g * sig
            hid_t[cols, :] = (silu * u).astype(BF16).T
            d_up = (d_hidden * silu).astype(BF16)
            d_gate = ((d_hidden * u) * (sig * (1.0 + g * (1.0 - sig)))).astype(BF16)
            du[:, cols] = d_up
            dg[:, cols] = d_gate
            du_t[cols, :] = d_up.T
            dg_t[cols, :] = d_gate.T
            return carry

        lax.fori_loop(0, ff // ff_tile, activate, 0)

        @pl.when(s > 0)
        def _():
            across_sum(s - 1).wait_send()

        def for_partner(j, carry):
            cols = columns(j)
            to_partner[:, cols] = term(dg[rows:, :], du[rows:, :], cols).astype(BF16)
            return carry

        lax.fori_loop(0, tiles, for_partner, 0)
        across_sum(s).start()

        @pl.when(s > 0)
        def _():
            gather_step(x_in, xg, xb, s, x_sems, loadx)

        def down(j, carry):
            cols = columns(j)
            acc_d[:, cols] += dot(hid_t[...], dyb[:, cols])
            return carry

        lax.fori_loop(0, tiles, down, 0)

        across_sum(s).wait_recv()
        theirs = pltpu.make_async_copy(partner_sums.at[s], dyb.at[pl.ds(rows, rows)], load.at[12])
        theirs.start()
        gather_rest(xg, xb, s, x_sems, loadx)

        def gate_up(j, carry):
            cols = columns(j)
            acc_g[:, cols] += dot(dg_t[...], xb[:, cols])
            acc_u[:, cols] += dot(du_t[...], xb[:, cols])
            return carry

        lax.fori_loop(0, tiles, gate_up, 0)

        slot = lax.div(s + n - 1, n)
        theirs.wait()

        def own(j, carry):
            cols = columns(j)
            terms[slot, :, cols] = term(dg[:rows, :], du[:rows, :], cols) + dyb[rows:, cols].astype(F32)
            return carry

        lax.fori_loop(0, tiles, own, 0)

        @pl.when(s == 0)
        def _():
            gather_step(dy_in, dyg, dyb, s + 1, dy_sems, load)

        @pl.when(s == 1)
        def _():
            def first(j, carry):
                cols = columns(j)
                to_ring[:, cols] = terms[1, :, cols].astype(BF16)
                return carry

            lax.fori_loop(0, tiles, first, 0)
            for h in range(2):
                for d in range(2):
                    ring_sum(s, d, h).start()

        @pl.when(s > 1)
        def _():
            add_arrived(s - 1, 1, dyb, True)

        return carry

    lax.fori_loop(0, n, step, 0)

    def finish_down(j, carry):
        cols = columns(j)
        dyb[:, cols] = acc_d[:, cols].astype(BF16)
        wg[cols, :] = acc_g[:, cols].astype(BF16).T
        wu[cols, :] = acc_u[:, cols].astype(BF16).T
        return carry

    lax.fori_loop(0, tiles, finish_down, 0)
    across_sum(n - 1).wait_send()

    def drain(s, carry):
        for mine, whole, sems in ((dy_in, dyg, dy_sems), (x_in, xg, x_sems)):
            for d in range(2):
                src = mine.at[pl.ds(d * half, half)]
                across(src, whole, s, d, sems).wait_send()

                @pl.when(s < n - 1)
                def _():
                    forward(src, whole, s, d, sems).wait_send()

        return carry

    lax.fori_loop(0, n, drain, 0)
    add_arrived(n - 1, 0, xb, False)


def solution(mesh):
    side = math.isqrt(mesh.shape["tp"] // 2)
    n = side * side
    assert 2 * n == mesh.shape["tp"]

    def step(x, dy, gate, up, w_gate, w_up, w_down):
        rows, depth = x.shape
        tokens, ff = gate.shape
        tile = min(512, depth)
        shape = jax.ShapeDtypeStruct
        any_space = pl.BlockSpec(memory_space=pl.ANY)
        dma = pltpu.SemaphoreType.DMA
        vmem = pltpu.VMEM
        outs = pl.pallas_call(
            functools.partial(kernel, side, tile),
            out_shape=[
                pltpu.VMEM((rows, depth), BF16),
                pltpu.VMEM((depth, ff), BF16),
                pltpu.VMEM((depth, ff), BF16),
                pltpu.VMEM((ff, depth), BF16),
                shape((tokens, depth), BF16),
                shape((tokens, depth), BF16),
                shape((n, 2, 2, rows // 4, depth), BF16),
                shape((n, rows, depth), BF16),
            ],
            in_specs=[any_space] * 7,
            out_specs=[pl.BlockSpec(memory_space=pltpu.VMEM)] * 4 + [any_space] * 4,
            scratch_shapes=[
                vmem((ff, depth), BF16),
                vmem((ff, depth), F32),
                vmem((ff, depth), F32),
                vmem((ff, depth), F32),
                vmem((2 * rows, depth), BF16),
                vmem((2 * rows, ff), BF16),
                vmem((2 * rows, ff), BF16),
                vmem((2 * rows, ff), BF16),
                vmem((2 * rows, ff), BF16),
                vmem((ff, 2 * rows), BF16),
                vmem((ff, 2 * rows), BF16),
                vmem((ff, 2 * rows), BF16),
                vmem((rows, depth), BF16),
                vmem((2, rows, depth), F32),
                dma((13,)),
                dma((3,)),
                dma((4,)),
            ]
            + [dma((2, n)), dma((2, n + 1)), dma((2, n)), dma((2, n))] * 2
            + [dma((4, n)), dma((4, n)), dma((n,)), dma((n,))],
            compiler_params=pltpu.CompilerParams(
                collective_id=0, has_side_effects=True, vmem_limit_bytes=48 * 2**20
            ),
        )(x, dy, gate, up, w_gate, w_up, w_down)
        return tuple(outs[:4])

    tokens_spec = P(("dp", "tp"), None)
    return jax.shard_map(
        step,
        mesh=mesh,
        in_specs=(tokens_spec, tokens_spec, P("dp", "tp"), P("dp", "tp"), P(None, "tp"), P(None, "tp"), P("tp", None)),
        out_specs=(tokens_spec, P("dp", "tp"), P("dp", "tp"), tokens_spec),
        check_vma=False,
    )
```

```python
import functools
import math

import jax
import jax.numpy as jnp
from jax import lax
from jax.experimental import pallas as pl
from jax.experimental.pallas import tpu as pltpu
from jax.sharding import PartitionSpec as P

MESH = pl.DeviceIdType.MESH
F32 = jnp.float32
BF16 = jnp.bfloat16
T_RHS = (((1,), (1,)), ((), ()))


def dot(a, b):
    return jnp.dot(a, b, preferred_element_type=F32)


def dot_t(a, b):
    return lax.dot_general(a, b, T_RHS, preferred_element_type=F32)


def kernel(
    side, tile,
    x_in, dy_in, gate, up, w_gate, w_up, w_down,
    to_ring, wg, wu, dyb, xg, dyg, sums, partner_sums,
    wd, acc_g, acc_u, acc_d, xb, gb, ub, dg, du, hid_t, dg_t, du_t, to_partner, terms,
    load, loadw, loadx,
    dy_s, dy_r, dy_ps, dy_pr, x_s, x_r, x_ps, x_pr, rs_s, rs_r, ps_s, ps_r,
):
    n = side * side
    rows, depth = x_in.shape
    half = rows // 2
    quarter = half // 2
    ff = gate.shape[1]
    tiles = depth // tile

    me = lax.axis_index("tp")
    core = lax.rem(me, 2)
    chip = lax.div(me, 2)
    cx, cy = lax.div(chip, side), lax.rem(chip, side)
    diagonal = lax.rem(cx + cy, side)

    def device(c, q):
        major = lax.div(q, side)
        minor = lax.rem(lax.rem(q, side) - major + side, side)
        x = major + c * (minor - major)
        y = minor + c * (major - minor)
        return (x * side + y) * 2 + c

    other = 1 - core
    place = (cx + core * (cy - cx)) * side + diagonal
    other_place = (cx + other * (cy - cx)) * side + diagonal
    right = device(core, lax.rem(place + 1, n))
    left = device(core, lax.rem(place + n - 1, n))
    partner = me + 1 - 2 * core
    onward = (right, left)

    def piece(s, i):
        c, at = (core, place) if i < 2 else (other, other_place)
        q = lax.rem(at + n - s, n) if i % 2 == 0 else lax.rem(at + s, n)
        return pl.multiple_of(device(c, q) * rows + (i % 2) * half, half)

    def remote(src, dst, send, recv, to):
        return pltpu.make_async_remote_copy(
            src_ref=src, dst_ref=dst, send_sem=send, recv_sem=recv, device_id={"tp": to}, device_id_type=MESH
        )

    def columns(j):
        return pl.ds(pl.multiple_of(j * tile, tile), tile)

    def forward(src, whole, s, d, sems):
        at = whole.at[pl.ds(piece(s, d), half)]
        return remote(src, at, sems[0].at[d, s], sems[1].at[d, s + 1], onward[d])

    def across(src, whole, s, d, sems):
        at = whole.at[pl.ds(piece(s, d), half)]
        return remote(src, at, sems[2].at[d, s], sems[3].at[d, s], partner)

    def arrived(whole, s, d, sems):
        at = whole.at[pl.ds(piece(s, d), half)]
        return remote(at, at, sems[0].at[d, s], sems[1].at[d, s], onward[d])

    def arrived_across(whole, s, d, sems):
        at = whole.at[pl.ds(piece(s, 2 + d), half)]
        return remote(at, at, sems[2].at[d, s], sems[3].at[d, s], partner)

    def chunk_load(src, buf, i, sem):
        return pltpu.make_async_copy(src, buf.at[pl.ds(i * half, half)], sem.at[i])

    def gather_step(mine, whole, buf, s, sems, sem):
        for d in range(2):

            @pl.when(s == 0)
            def _():
                src = mine.at[pl.ds(d * half, half)]
                forward(src, whole, s, d, sems).start()
                across(src, whole, s, d, sems).start()
                chunk_load(src, buf, d, sem).start()

            @pl.when(s > 0)
            def _():
                arrived(whole, s, d, sems).wait_recv()
                src = whole.at[pl.ds(piece(s, d), half)]

                @pl.when(s < n - 1)
                def _():
                    forward(src, whole, s, d, sems).start()

                across(src, whole, s, d, sems).start()
                chunk_load(src, buf, d, sem).start()

    def gather_rest(whole, buf, s, sems, sem):
        for d in range(2):
            arrived_across(whole, s, d, sems).wait_recv()
            chunk_load(whole.at[pl.ds(piece(s, 2 + d), half)], buf, 2 + d, sem).start()
        for i in range(4):
            chunk_load(whole.at[pl.ds(piece(s, i), half)], buf, i, sem).wait()

    dy_sems = (dy_s, dy_r, dy_ps, dy_pr)
    x_sems = (x_s, x_r, x_ps, x_pr)

    def across_sum(s):
        return remote(to_partner, partner_sums.at[s], ps_s.at[s], ps_r.at[s], partner)

    def ring_sum(s, d, h):
        src = to_ring.at[pl.ds(d * half + h * quarter, quarter)]
        return remote(src, sums.at[s, d, h], rs_s.at[2 * d + h, s], rs_r.at[2 * d + h, s], onward[d])

    def theirs_load(s, buf):
        return pltpu.make_async_copy(partner_sums.at[s], buf.at[pl.ds(rows, rows)], load.at[12])

    def add_arrived(s, term_slot, buf, send):
        def incoming(d, h):
            at = pl.ds(d * half + h * quarter, quarter)
            return pltpu.make_async_copy(sums.at[last(s), d, h], buf.at[at], load.at[d])

        def last(s):
            return s - 1 if send else n - 1

        for h in range(2):
            for d in range(2):
                ring_sum(last(s), d, h).wait_recv()
                incoming(d, h).start()
            if h == 0:
                theirs_load(s, buf).wait()
            for d in range(2):
                ring_sum(last(s), d, h).wait_send()
                incoming(d, h).wait()
                at = pl.ds(d * half + h * quarter, quarter)
                across_at = pl.ds(rows + d * half + h * quarter, quarter)

                def add(j, carry):
                    cols = columns(j)
                    total = terms[term_slot, at, cols] + buf[across_at, cols].astype(F32) + buf[at, cols].astype(F32)
                    to_ring[at, cols] = total.astype(BF16)
                    return carry

                lax.fori_loop(0, tiles, add, 0)
                if send:
                    ring_sum(s, d, h).start()

    def term(a_gate, a_up, cols):
        return dot_t(a_gate, wg[cols, :]) + dot_t(a_up, wu[cols, :])

    def weight_loads():
        return [pltpu.make_async_copy(src, dst, loadw.at[i]) for i, (src, dst) in enumerate(((w_down, wd), (w_gate, wg), (w_up, wu)))]

    barrier = pltpu.get_barrier_semaphore()
    for peer in (left, right, partner):
        pl.semaphore_signal(barrier, inc=1, device_id={"tp": peer}, device_id_type=MESH)
    pl.semaphore_wait(barrier, 3)

    def step(s, carry):
        kept = []
        for i in range(4):
            at = pl.ds(piece(s, i), half)
            kept.append(pltpu.make_async_copy(gate.at[at], gb.at[pl.ds(i * half, half)], load.at[4 + i]))
            kept.append(pltpu.make_async_copy(up.at[at], ub.at[pl.ds(i * half, half)], load.at[8 + i]))
        for copy in kept:
            copy.start()

        @pl.when(s != 1)
        def _():
            gather_step(dy_in, dyg, dyb, s, dy_sems, load)

        @pl.when(s == 0)
        def _():
            for copy in weight_loads():
                copy.start()

            def clear(j, carry):
                zero = jnp.zeros((ff, tile), F32)
                for acc in (acc_g, acc_u, acc_d):
                    acc[:, columns(j)] = zero
                return carry

            gather_step(x_in, xg, xb, s, x_sems, loadx)
            lax.fori_loop(0, tiles, clear, 0)
            for copy in weight_loads():
                copy.wait()

        gather_rest(dyg, dyb, s, dy_sems, load)
        for copy in kept:
            copy.wait()

        ff_tile = min(256, ff)

        def activate(j, carry):
            cols = pl.ds(pl.multiple_of(j * ff_tile, ff_tile), ff_tile)
            d_hidden = dot_t(dyb[...], wd[cols, :])
            g, u = gb[:, cols].astype(F32), ub[:, cols].astype(F32)
            sig = jax.nn.sigmoid(g)
            silu = g * sig
            hid_t[cols, :] = (silu * u).astype(BF16).T
            d_up = (d_hidden * silu).astype(BF16)
            d_gate = ((d_hidden * u) * (sig * (1.0 + g * (1.0 - sig)))).astype(BF16)
            du[:, cols] = d_up
            dg[:, cols] = d_gate
            du_t[cols, :] = d_up.T
            dg_t[cols, :] = d_gate.T
            return carry

        lax.fori_loop(0, ff // ff_tile, activate, 0)

        slot = lax.div(s + n - 1, n)

        @pl.when(s > 0)
        def _():
            across_sum(s - 1).wait_send()

        def own_terms(j, carry):
            cols = columns(j)
            both = term(dg[...], du[...], cols)
            to_partner[:, cols] = both[rows:].astype(BF16)
            terms[slot, :, cols] = both[:rows]
            return carry

        lax.fori_loop(0, tiles, own_terms, 0)
        across_sum(s).start()

        @pl.when(s > 0)
        def _():
            gather_step(x_in, xg, xb, s, x_sems, loadx)

        def down(j, carry):
            cols = columns(j)
            acc_d[:, cols] += dot(hid_t[...], dyb[:, cols])
            return carry

        lax.fori_loop(0, tiles, down, 0)

        @pl.when(s == 0)
        def _():
            gather_step(dy_in, dyg, dyb, s + 1, dy_sems, load)

        @pl.when(s == 1)
        def _():
            across_sum(s).wait_recv()
            theirs_load(s, dyb).start()
            theirs_load(s, dyb).wait()

            def first(j, carry):
                cols = columns(j)
                to_ring[:, cols] = (terms[1, :, cols] + dyb[rows:, cols].astype(F32)).astype(BF16)
                return carry

            lax.fori_loop(0, tiles, first, 0)
            for h in range(2):
                for d in range(2):
                    ring_sum(s, d, h).start()

        @pl.when(s > 1)
        def _():
            across_sum(s).wait_recv()
            theirs_load(s, dyb).start()
            add_arrived(s, 1, dyb, True)

        gather_rest(xg, xb, s, x_sems, loadx)

        def gate_up(j, carry):
            cols = columns(j)
            acc_g[:, cols] += dot(dg_t[...], xb[:, cols])
            acc_u[:, cols] += dot(du_t[...], xb[:, cols])
            return carry

        lax.fori_loop(0, tiles, gate_up, 0)

        return carry

    lax.fori_loop(0, n, step, 0)

    across_sum(0).wait_recv()
    theirs_load(0, xb).start()

    def finish_down(j, carry):
        cols = columns(j)
        dyb[:, cols] = acc_d[:, cols].astype(BF16)
        wg[cols, :] = acc_g[:, cols].astype(BF16).T
        wu[cols, :] = acc_u[:, cols].astype(BF16).T
        return carry

    lax.fori_loop(0, tiles, finish_down, 0)
    across_sum(n - 1).wait_send()

    def drain(s, carry):
        for mine, whole, sems in ((dy_in, dyg, dy_sems), (x_in, xg, x_sems)):
            for d in range(2):
                src = mine.at[pl.ds(d * half, half)]
                across(src, whole, s, d, sems).wait_send()

                @pl.when(s < n - 1)
                def _():
                    forward(src, whole, s, d, sems).wait_send()

        return carry

    lax.fori_loop(0, n, drain, 0)
    add_arrived(0, 0, xb, False)


def solution(mesh):
    side = math.isqrt(mesh.shape["tp"] // 2)
    n = side * side
    assert 2 * n == mesh.shape["tp"]

    def step(x, dy, gate, up, w_gate, w_up, w_down):
        rows, depth = x.shape
        tokens, ff = gate.shape
        tile = min(512, depth)
        shape = jax.ShapeDtypeStruct
        any_space = pl.BlockSpec(memory_space=pl.ANY)
        dma = pltpu.SemaphoreType.DMA
        vmem = pltpu.VMEM
        outs = pl.pallas_call(
            functools.partial(kernel, side, tile),
            out_shape=[
                pltpu.VMEM((rows, depth), BF16),
                pltpu.VMEM((depth, ff), BF16),
                pltpu.VMEM((depth, ff), BF16),
                pltpu.VMEM((ff, depth), BF16),
                shape((tokens, depth), BF16),
                shape((tokens, depth), BF16),
                shape((n, 2, 2, rows // 4, depth), BF16),
                shape((n, rows, depth), BF16),
            ],
            in_specs=[any_space] * 7,
            out_specs=[pl.BlockSpec(memory_space=pltpu.VMEM)] * 4 + [any_space] * 4,
            scratch_shapes=[
                vmem((ff, depth), BF16),
                vmem((ff, depth), F32),
                vmem((ff, depth), F32),
                vmem((ff, depth), F32),
                vmem((2 * rows, depth), BF16),
                vmem((2 * rows, ff), BF16),
                vmem((2 * rows, ff), BF16),
                vmem((2 * rows, ff), BF16),
                vmem((2 * rows, ff), BF16),
                vmem((ff, 2 * rows), BF16),
                vmem((ff, 2 * rows), BF16),
                vmem((ff, 2 * rows), BF16),
                vmem((rows, depth), BF16),
                vmem((2, rows, depth), F32),
                dma((13,)),
                dma((3,)),
                dma((4,)),
            ]
            + [dma((2, n)), dma((2, n + 1)), dma((2, n)), dma((2, n))] * 2
            + [dma((4, n)), dma((4, n)), dma((n,)), dma((n,))],
            compiler_params=pltpu.CompilerParams(
                collective_id=0, has_side_effects=True, vmem_limit_bytes=48 * 2**20
            ),
        )(x, dy, gate, up, w_gate, w_up, w_down)
        return tuple(outs[:4])

    tokens_spec = P(("dp", "tp"), None)
    return jax.shard_map(
        step,
        mesh=mesh,
        in_specs=(tokens_spec, tokens_spec, P("dp", "tp"), P("dp", "tp"), P(None, "tp"), P(None, "tp"), P("tp", None)),
        out_specs=(tokens_spec, P("dp", "tp"), P("dp", "tp"), tokens_spec),
        check_vma=False,
    )
```

```python
import functools
import math

import jax
import jax.numpy as jnp
from jax import lax
from jax.experimental import pallas as pl
from jax.experimental.pallas import tpu as pltpu
from jax.sharding import PartitionSpec as P

MESH = pl.DeviceIdType.MESH
F32 = jnp.float32
BF16 = jnp.bfloat16
T_RHS = (((1,), (1,)), ((), ()))


def dot(a, b):
    return jnp.dot(a, b, preferred_element_type=F32)


def dot_t(a, b):
    return lax.dot_general(a, b, T_RHS, preferred_element_type=F32)


def kernel(
    side, tile,
    x_in, dy_in, gate, up, w_gate, w_up, w_down,
    to_ring, wg, wu, dyb, xg, dyg, sums, partner_sums,
    wd, acc_g, acc_u, acc_d, xb, gb, ub, dg, du, hid_t, dg_t, du_t, to_partner, terms, landed,
    load, loadw, loadx,
    dy_s, dy_r, dy_ps, dy_pr, x_s, x_r, x_ps, x_pr, rs_s, rs_r, ps_s, ps_r,
):
    n = side * side
    rows, depth = x_in.shape
    half = rows // 2
    quarter = half // 2
    ff = gate.shape[1]
    tiles = depth // tile

    me = lax.axis_index("tp")
    core = lax.rem(me, 2)
    chip = lax.div(me, 2)
    cx, cy = lax.div(chip, side), lax.rem(chip, side)
    diagonal = lax.rem(cx + cy, side)

    def device(c, q):
        major = lax.div(q, side)
        minor = lax.rem(lax.rem(q, side) - major + side, side)
        x = major + c * (minor - major)
        y = minor + c * (major - minor)
        return (x * side + y) * 2 + c

    other = 1 - core
    place = (cx + core * (cy - cx)) * side + diagonal
    other_place = (cx + other * (cy - cx)) * side + diagonal
    right = device(core, lax.rem(place + 1, n))
    left = device(core, lax.rem(place + n - 1, n))
    partner = me + 1 - 2 * core
    onward = (right, left)

    def piece(s, i):
        c, at = (core, place) if i < 2 else (other, other_place)
        q = lax.rem(at + n - s, n) if i % 2 == 0 else lax.rem(at + s, n)
        return pl.multiple_of(device(c, q) * rows + (i % 2) * half, half)

    def remote(src, dst, send, recv, to):
        return pltpu.make_async_remote_copy(
            src_ref=src, dst_ref=dst, send_sem=send, recv_sem=recv, device_id={"tp": to}, device_id_type=MESH
        )

    def columns(j):
        return pl.ds(pl.multiple_of(j * tile, tile), tile)

    def forward(src, whole, s, d, sems):
        at = whole.at[pl.ds(piece(s, d), half)]
        return remote(src, at, sems[0].at[d, s], sems[1].at[d, s + 1], onward[d])

    def across(src, whole, s, d, sems):
        at = whole.at[pl.ds(piece(s, d), half)]
        return remote(src, at, sems[2].at[d, s], sems[3].at[d, s], partner)

    def arrived(whole, s, d, sems):
        at = whole.at[pl.ds(piece(s, d), half)]
        return remote(at, at, sems[0].at[d, s], sems[1].at[d, s], onward[d])

    def arrived_across(whole, s, d, sems):
        at = whole.at[pl.ds(piece(s, 2 + d), half)]
        return remote(at, at, sems[2].at[d, s], sems[3].at[d, s], partner)

    def chunk_load(src, buf, i, sem):
        return pltpu.make_async_copy(src, buf.at[pl.ds(i * half, half)], sem.at[i])

    def gather_step(mine, whole, buf, s, sems, sem):
        for d in range(2):

            @pl.when(s == 0)
            def _():
                src = mine.at[pl.ds(d * half, half)]
                forward(src, whole, s, d, sems).start()
                across(src, whole, s, d, sems).start()
                chunk_load(src, buf, d, sem).start()

            @pl.when(s > 0)
            def _():
                arrived(whole, s, d, sems).wait_recv()
                src = whole.at[pl.ds(piece(s, d), half)]

                @pl.when(s < n - 1)
                def _():
                    forward(src, whole, s, d, sems).start()

                across(src, whole, s, d, sems).start()
                chunk_load(src, buf, d, sem).start()

    def gather_rest(whole, buf, s, sems, sem):
        for d in range(2):
            arrived_across(whole, s, d, sems).wait_recv()
            chunk_load(whole.at[pl.ds(piece(s, 2 + d), half)], buf, 2 + d, sem).start()
        for i in range(4):
            chunk_load(whole.at[pl.ds(piece(s, i), half)], buf, i, sem).wait()

    dy_sems = (dy_s, dy_r, dy_ps, dy_pr)
    x_sems = (x_s, x_r, x_ps, x_pr)

    def across_sum(s):
        return remote(to_partner, partner_sums.at[s], ps_s.at[s], ps_r.at[s], partner)

    def ring_sum(s, d, h):
        src = to_ring.at[pl.ds(d * half + h * quarter, quarter)]
        return remote(src, sums.at[s, d, h], rs_s.at[2 * d + h, s], rs_r.at[2 * d + h, s], onward[d])

    def last_sum(d, h):
        at = pl.ds(d * half + h * quarter, quarter)
        return remote(to_ring.at[at], landed.at[at], rs_s.at[2 * d + h, n - 1], rs_r.at[2 * d + h, n - 1], onward[d])

    def theirs_load(s, buf):
        return pltpu.make_async_copy(partner_sums.at[s], buf.at[pl.ds(rows, rows)], load.at[12])

    def sum_up(slot, d, h, arrived, theirs):
        at = pl.ds(d * half + h * quarter, quarter)
        theirs_at = pl.ds(rows + d * half + h * quarter, quarter)

        def add(j, carry):
            cols = columns(j)
            total = terms[slot, at, cols] + theirs[theirs_at, cols].astype(F32) + arrived[at, cols].astype(F32)
            to_ring[at, cols] = total.astype(BF16)
            return carry

        lax.fori_loop(0, tiles, add, 0)

    def add_arrived(s):
        def incoming(d, h):
            at = pl.ds(d * half + h * quarter, quarter)
            return pltpu.make_async_copy(sums.at[s - 1, d, h], dyb.at[at], load.at[d])

        for h in range(2):
            for d in range(2):
                ring_sum(s - 1, d, h).wait_recv()
                incoming(d, h).start()
            if h == 0:
                theirs_load(s, dyb).wait()
            for d in range(2):
                ring_sum(s - 1, d, h).wait_send()
                incoming(d, h).wait()
                sum_up(1, d, h, dyb, dyb)

                @pl.when(s < n - 1)
                def _():
                    ring_sum(s, d, h).start()

                @pl.when(s == n - 1)
                def _():
                    last_sum(d, h).start()

    def term(a_gate, a_up, cols):
        return dot_t(a_gate, wg[cols, :]) + dot_t(a_up, wu[cols, :])

    def weight_loads():
        return [pltpu.make_async_copy(src, dst, loadw.at[i]) for i, (src, dst) in enumerate(((w_down, wd), (w_gate, wg), (w_up, wu)))]

    barrier = pltpu.get_barrier_semaphore()
    for peer in (left, right, partner):
        pl.semaphore_signal(barrier, inc=1, device_id={"tp": peer}, device_id_type=MESH)
    pl.semaphore_wait(barrier, 3)

    def step(s, carry):
        kept = []
        for i in range(4):
            at = pl.ds(piece(s, i), half)
            kept.append(pltpu.make_async_copy(gate.at[at], gb.at[pl.ds(i * half, half)], load.at[4 + i]))
            kept.append(pltpu.make_async_copy(up.at[at], ub.at[pl.ds(i * half, half)], load.at[8 + i]))
        for copy in kept:
            copy.start()

        @pl.when(s != 1)
        def _():
            gather_step(dy_in, dyg, dyb, s, dy_sems, load)

        @pl.when(s == 0)
        def _():
            for copy in weight_loads():
                copy.start()

            def clear(j, carry):
                zero = jnp.zeros((ff, tile), F32)
                for acc in (acc_g, acc_u, acc_d):
                    acc[:, columns(j)] = zero
                return carry

            gather_step(x_in, xg, xb, s, x_sems, loadx)
            lax.fori_loop(0, tiles, clear, 0)
            for copy in weight_loads():
                copy.wait()

        gather_rest(dyg, dyb, s, dy_sems, load)
        for copy in kept:
            copy.wait()

        ff_tile = min(256, ff)

        def activate(j, carry):
            cols = pl.ds(pl.multiple_of(j * ff_tile, ff_tile), ff_tile)
            d_hidden = dot_t(dyb[...], wd[cols, :])
            g, u = gb[:, cols].astype(F32), ub[:, cols].astype(F32)
            sig = jax.nn.sigmoid(g)
            silu = g * sig
            hid_t[cols, :] = (silu * u).astype(BF16).T
            d_up = (d_hidden * silu).astype(BF16)
            d_gate = ((d_hidden * u) * (sig * (1.0 + g * (1.0 - sig)))).astype(BF16)
            du[:, cols] = d_up
            dg[:, cols] = d_gate
            du_t[cols, :] = d_up.T
            dg_t[cols, :] = d_gate.T
            return carry

        lax.fori_loop(0, ff // ff_tile, activate, 0)

        @pl.when(s > 0)
        def _():
            gather_step(x_in, xg, xb, s, x_sems, loadx)

        slot = lax.div(s + n - 1, n)

        @pl.when(s > 0)
        def _():
            across_sum(s - 1).wait_send()

        def own_terms(j, carry):
            cols = columns(j)
            both = term(dg[...], du[...], cols)
            to_partner[:, cols] = both[rows:].astype(BF16)
            terms[slot, :, cols] = both[:rows]
            return carry

        lax.fori_loop(0, tiles, own_terms, 0)
        across_sum(s).start()

        def down(j, carry):
            cols = columns(j)
            acc_d[:, cols] += dot(hid_t[...], dyb[:, cols])
            return carry

        lax.fori_loop(0, tiles, down, 0)

        @pl.when(s == 0)
        def _():
            gather_step(dy_in, dyg, dyb, s + 1, dy_sems, load)

        @pl.when(s == 1)
        def _():
            across_sum(s).wait_recv()
            theirs_load(s, dyb).start()
            theirs_load(s, dyb).wait()

            def first(j, carry):
                cols = columns(j)
                to_ring[:, cols] = (terms[1, :, cols] + dyb[rows:, cols].astype(F32)).astype(BF16)
                return carry

            lax.fori_loop(0, tiles, first, 0)
            for h in range(2):
                for d in range(2):
                    ring_sum(s, d, h).start()

        @pl.when(s > 1)
        def _():
            across_sum(s).wait_recv()
            theirs_load(s, dyb).start()
            add_arrived(s)

        gather_rest(xg, xb, s, x_sems, loadx)

        def gate_up(j, carry):
            cols = columns(j)
            acc_g[:, cols] += dot(dg_t[...], xb[:, cols])
            acc_u[:, cols] += dot(du_t[...], xb[:, cols])
            return carry

        lax.fori_loop(0, tiles, gate_up, 0)

        return carry

    lax.fori_loop(0, n, step, 0)

    across_sum(0).wait_recv()
    theirs_load(0, xb).start()

    def finish_down(j, carry):
        cols = columns(j)
        dyb[:, cols] = acc_d[:, cols].astype(BF16)
        wg[cols, :] = acc_g[:, cols].astype(BF16).T
        wu[cols, :] = acc_u[:, cols].astype(BF16).T
        return carry

    lax.fori_loop(0, tiles, finish_down, 0)
    across_sum(n - 1).wait_send()

    def drain(s, carry):
        for mine, whole, sems in ((dy_in, dyg, dy_sems), (x_in, xg, x_sems)):
            for d in range(2):
                src = mine.at[pl.ds(d * half, half)]
                across(src, whole, s, d, sems).wait_send()

                @pl.when(s < n - 1)
                def _():
                    forward(src, whole, s, d, sems).wait_send()

        return carry

    lax.fori_loop(0, n, drain, 0)
    theirs_load(0, xb).wait()
    for h in range(2):
        for d in range(2):
            last_sum(d, h).wait()
            sum_up(0, d, h, landed, xb)


def store(*refs):
    held, out, sem = refs[:4], refs[4:8], refs[8]
    copies = [pltpu.make_async_copy(a, b, sem.at[i]) for i, (a, b) in enumerate(zip(held, out))]
    for copy in copies:
        copy.start()
    for copy in copies:
        copy.wait()


def solution(mesh):
    side = math.isqrt(mesh.shape["tp"] // 2)
    n = side * side
    assert 2 * n == mesh.shape["tp"]

    def step(x, dy, gate, up, w_gate, w_up, w_down):
        rows, depth = x.shape
        tokens, ff = gate.shape
        tile = min(512, depth)
        shape = jax.ShapeDtypeStruct
        any_space = pl.BlockSpec(memory_space=pl.ANY)
        dma = pltpu.SemaphoreType.DMA
        vmem = pltpu.VMEM
        outs = pl.pallas_call(
            functools.partial(kernel, side, tile),
            out_shape=[
                pltpu.VMEM((rows, depth), BF16),
                pltpu.VMEM((depth, ff), BF16),
                pltpu.VMEM((depth, ff), BF16),
                pltpu.VMEM((ff, depth), BF16),
                shape((tokens, depth), BF16),
                shape((tokens, depth), BF16),
                shape((n, 2, 2, rows // 4, depth), BF16),
                shape((n, rows, depth), BF16),
            ],
            in_specs=[any_space] * 7,
            out_specs=[pl.BlockSpec(memory_space=pltpu.VMEM)] * 4 + [any_space] * 4,
            scratch_shapes=[
                vmem((ff, depth), BF16),
                vmem((ff, depth), F32),
                vmem((ff, depth), F32),
                vmem((ff, depth), F32),
                vmem((2 * rows, depth), BF16),
                vmem((2 * rows, ff), BF16),
                vmem((2 * rows, ff), BF16),
                vmem((2 * rows, ff), BF16),
                vmem((2 * rows, ff), BF16),
                vmem((ff, 2 * rows), BF16),
                vmem((ff, 2 * rows), BF16),
                vmem((ff, 2 * rows), BF16),
                vmem((rows, depth), BF16),
                vmem((2, rows, depth), F32),
                vmem((rows, depth), BF16),
                dma((13,)),
                dma((3,)),
                dma((4,)),
            ]
            + [dma((2, n)), dma((2, n + 1)), dma((2, n)), dma((2, n))] * 2
            + [dma((4, n)), dma((4, n)), dma((n,)), dma((n,))],
            compiler_params=pltpu.CompilerParams(
                collective_id=0, has_side_effects=True, vmem_limit_bytes=199 * 2**18
            ),
        )(x, dy, gate, up, w_gate, w_up, w_down)
        return pl.pallas_call(
            store,
            out_shape=[shape(out.shape, BF16) for out in outs[:4]],
            in_specs=[pl.BlockSpec(memory_space=vmem)] * 4,
            out_specs=[any_space] * 4,
            scratch_shapes=[dma((4,))],
            compiler_params=pltpu.CompilerParams(vmem_limit_bytes=2**20),
        )(*[pltpu.with_memory_space_constraint(out, vmem) for out in outs[:4]])

    tokens_spec = P(("dp", "tp"), None)
    return jax.shard_map(
        step,
        mesh=mesh,
        in_specs=(tokens_spec, tokens_spec, P("dp", "tp"), P("dp", "tp"), P(None, "tp"), P(None, "tp"), P("tp", None)),
        out_specs=(tokens_spec, P("dp", "tp"), P("dp", "tp"), tokens_spec),
        check_vma=False,
    )
```
